256 devices in a mesh: tbl: 64 (over y, z, core), pair: 4 (over x).
Axes of the slice: x: 4, y: 4, z: 8, core: 2. Of those that a mesh axis runs over, the one named last changes fastest.
Arguments:
- codes: bfloat16 [128, 64, 131072], P('tbl', None, 'pair'), may hold values from -127 to 127
- scales: float32 [128, 131072], P('tbl', 'pair'), may hold values from 0.002 to 0.02
- shard_slot: int32 [64, 2], replicated, may hold values from -1 to 53, as said below
- weight_first: bfloat16 [351, 1024], replicated, may hold values from -0.3125 to 0.3125
- bias_first: float32 [1024], replicated, may hold values from -3 to 3
- weight_second: bfloat16 [1024, 1024], replicated, may hold values from -0.1875 to 0.1875
- bias_second: float32 [1024], replicated, may hold values from -3 to 3
- weight_third: bfloat16 [1024, 512], replicated, may hold values from -0.1875 to 0.1875
- bias_third: float32 [512], replicated, may hold values from -3 to 3
- weight_fourth: bfloat16 [512, 256], replicated, may hold values from -0.25 to 0.25
- bias_fourth: float32 [256], replicated, may hold values from -3 to 3
- weight_out: bfloat16 [256], replicated, may hold values from -0.375 to 0.375
- bias_out: float32 [1], replicated, may hold values from -3 to 3
Outputs:
- logits: float32 [4, 32768], P(None, 'tbl')
The draws below stay inside these ranges and needn't reach their ends.
Inputs may be any that keep to these rules, and one draw needn't show every extreme that they name: `shard_slot`: each shard 0 to 53 stands in exactly one slot; all other slots hold -1. For k below half of the tbl size, row k holds its shards in its first slots and the row half the tbl size further holds its shards in its last slots, and the two rows hold 2 shards or fewer together. Some row holds 2 shards.
All inputs are finite; a program needn't handle non-finite values.
Results may differ from the reference program's by a relative error of at most 0.03.
Values may be sent and summed in bfloat16 or wider, within the bound.
A program may use at most 128 MiB of HBM per device.

```python
import math
import jax
import jax.numpy as jnp
import numpy as np
from jax import lax

TABLES = 27
TOP_ONE = 1024
TOP_TWO = 1024
TOP_THREE = 512
TOP_FOUR = 256
HALF = 64
SHARDS = 54
PAIRS = 351
SLOTS = 2
BATCH_PAIR = 32768
BATCH = 131072
N_TBL = 64
N_PAIR = 4


def draw_shard_slot(key, part):
    span = N_TBL // 2
    key_rank, key_split, key_order = jax.random.split(jax.random.fold_in(key, 71), 3)
    rank = jax.random.permutation(key_rank, span).astype(jnp.int32)
    count = jnp.clip(SHARDS - rank * SLOTS, 0, SLOTS)
    lower = jax.random.randint(key_split, (span,), 0, SLOTS + 1)
    lower = jnp.minimum(lower, count)
    lower = jnp.where(rank == 0, count, lower)
    order = jax.random.permutation(key_order, SHARDS).astype(jnp.int32)
    padded = jnp.concatenate([order, jnp.zeros((span * SLOTS - SHARDS,), jnp.int32)])
    slot_index = jnp.arange(SLOTS, dtype=jnp.int32)
    low_place = rank[:, None] * SLOTS + slot_index[None, :]
    low_valid = slot_index[None, :] < lower[:, None]
    upper_count = count - lower
    upper_start = SLOTS - upper_count
    high_place = rank[:, None] * SLOTS + lower[:, None] + slot_index[None, :] - upper_start[:, None]
    high_valid = slot_index[None, :] >= upper_start[:, None]
    limit = span * SLOTS - 1
    low_rows = jnp.where(low_valid, padded[jnp.clip(low_place, 0, limit)], -1)
    high_rows = jnp.where(high_valid, padded[jnp.clip(high_place, 0, limit)], -1)
    return jnp.concatenate([low_rows, high_rows], axis=0).astype(jnp.int32)


def level_of(rng, extent, pieces, smallest, top_value):
    gain, own = 1.0, jax.random.fold_in(rng, 6)
    for dim, shards_of in pieces:
        heights = jnp.exp(jax.random.uniform(jax.random.fold_in(own, dim), (shards_of,), jnp.float32, smallest / len(pieces), top_value / len(pieces)))
        gain = gain * jnp.repeat(heights, extent[dim] // shards_of).reshape([-1 if axis == dim else 1 for axis in range(len(extent))])
    return gain


def gaussian(rng, dims, spread, reach, kind=jnp.bfloat16):
    array = spread * jax.random.normal(rng, dims, jnp.float32)
    return jnp.clip(array, min=-reach, max=reach).astype(kind)


def setup_inputs(seed: int = 0) -> dict:
    arg_keys = jax.random.split(jax.random.key(seed), 14)
    codes = jnp.clip(jax.random.uniform(arg_keys[0], (N_TBL * SLOTS, HALF, BATCH), jnp.float32, -127.0, 127.0) * level_of(arg_keys[0], (N_TBL * SLOTS, HALF, BATCH), ((0, 64), (2, 4)), -0.4, 0.0), -127.0, 127.0).astype(jnp.bfloat16)
    scales = jnp.clip(jnp.exp(math.log(0.02) - 2.30258502 * jax.random.uniform(arg_keys[1], (N_TBL * SLOTS, BATCH), jnp.float32) ** level_of(arg_keys[1], (N_TBL * SLOTS, BATCH), ((0, 64), (1, 4)), -0.2, 0.2)), 0.002, 0.02)
    shard_slot = draw_shard_slot(jax.random.fold_in(arg_keys[13], 71), 0)
    weight_first = gaussian(arg_keys[3], (PAIRS, TOP_ONE), PAIRS ** -0.5, 0.3125)
    bias_first = gaussian(arg_keys[4], (TOP_ONE,), 0.5, 3.0, jnp.float32)
    weight_second = gaussian(arg_keys[5], (TOP_ONE, TOP_TWO), TOP_ONE ** -0.5, 0.1875)
    bias_second = gaussian(arg_keys[6], (TOP_TWO,), 0.5, 3.0, jnp.float32)
    weight_third = gaussian(arg_keys[7], (TOP_TWO, TOP_THREE), TOP_TWO ** -0.5, 0.1875)
    bias_third = gaussian(arg_keys[8], (TOP_THREE,), 0.5, 3.0, jnp.float32)
    weight_fourth = gaussian(arg_keys[9], (TOP_THREE, TOP_FOUR), TOP_THREE ** -0.5, 0.25)
    bias_fourth = gaussian(arg_keys[10], (TOP_FOUR,), 0.5, 3.0, jnp.float32)
    weight_out = gaussian(arg_keys[11], (TOP_FOUR,), TOP_FOUR ** -0.5, 0.375)
    bias_out = gaussian(arg_keys[12], (1,), 1.0, 3.0, jnp.float32)
    return dict(codes=codes, scales=scales, shard_slot=shard_slot, weight_first=weight_first, bias_first=bias_first, weight_second=weight_second, bias_second=bias_second, weight_third=weight_third, bias_third=bias_third, weight_fourth=weight_fourth, bias_fourth=bias_fourth, weight_out=weight_out, bias_out=bias_out)


def pair_columns(tables):
    first, second = np.triu_indices(tables, 1)
    return (first * tables + second).astype(np.int32)


def shard_positions(slot_table, shard_total):
    flat = slot_table.reshape(-1)
    matches = flat[None, :] == jnp.arange(shard_total, dtype=jnp.int32)[:, None]
    places = jnp.arange(flat.shape[0], dtype=jnp.int32)[None, :]
    return jnp.sum(jnp.where(matches, places, 0), axis=1).astype(jnp.int32)


def dense_layer(inputs, weight, bias):
    product = jnp.dot(inputs.astype(jnp.float32), weight.astype(jnp.float32), precision=lax.Precision.HIGHEST)
    return jax.nn.relu(product + bias).astype(jnp.bfloat16)


def score_samples(picked_codes, picked_scales, layers):
    values = picked_codes.astype(jnp.float32) * picked_scales[:, None, :]
    table_count = values.shape[0] // 2
    count = values.shape[2]
    values = values.reshape(table_count, 2 * values.shape[1], count)
    gram = jnp.einsum("idb,jdb->bij", values, values, precision=lax.Precision.HIGHEST)
    flat = gram.reshape(count, table_count * table_count)
    hidden = flat[:, pair_columns(table_count)].astype(jnp.bfloat16)
    for weight, bias in layers[:-1]:
        hidden = dense_layer(hidden, weight, bias)
    weight_last, bias_last = layers[-1]
    final = jnp.dot(hidden.astype(jnp.float32), weight_last.astype(jnp.float32), precision=lax.Precision.HIGHEST)
    return final + bias_last[0]


def reference(codes, scales, shard_slot, weight_first, bias_first, weight_second, bias_second, weight_third, bias_third, weight_fourth, bias_fourth, weight_out, bias_out):
    layers = ((weight_first, bias_first), (weight_second, bias_second), (weight_third, bias_third), (weight_fourth, bias_fourth), (weight_out, bias_out))
    positions = shard_positions(shard_slot, 2 * TABLES)
    picked_codes = jnp.take(codes, positions, axis=0)
    picked_scales = jnp.take(scales, positions, axis=0)

    def block(index):
        start = index * BATCH_PAIR
        block_codes = lax.dynamic_slice_in_dim(picked_codes, start, BATCH_PAIR, 2)
        block_scales = lax.dynamic_slice_in_dim(picked_scales, start, BATCH_PAIR, 1)
        return score_samples(block_codes, block_scales, layers)

    logits = lax.map(block, jnp.arange(BATCH // BATCH_PAIR, dtype=jnp.int32))
    return logits.reshape(N_PAIR, BATCH_PAIR)
```

```python
import functools

import jax
import jax.numpy as jnp
from jax import lax
from jax.experimental import pallas as pl
from jax.experimental.pallas import tpu as pltpu
from jax.sharding import PartitionSpec as P

MESH = pl.DeviceIdType.MESH
F32 = jnp.float32
BF16 = jnp.bfloat16

TABLES = 27
SHIFTS = TABLES // 2
PAIRS = TABLES * SHIFTS
NY, NZC, NX = 4, 16, 4
NQ, NG = 4, 4
CHUNKS = NQ * NG
AHEAD = 4
LAG = 2
Z_ORDER = (4, 3, 5, 2, 6, 1, 7)


def kernel(
    slot_ref,
    place_ref,
    bout_ref,
    codes,
    scales,
    w1,
    b1,
    w2,
    b2,
    w3,
    b3,
    w4,
    b4,
    wout_ref,
    out_ref,
    y_recv,
    merged,
    z_recv,
    sc_in,
    sc_send,
    y_sc,
    m_sc,
    z_sc,
    sc,
    unit,
    vals,
    acc,
    xt,
    lg,
    w1v,
    w1p,
    b1v,
    w2v,
    b2v,
    w3v,
    b3v,
    w4v,
    b4v,
    y_ssem,
    y_rsem,
    z_ssem,
    z_rsem,
    sc_ssem,
    sc_rsem,
    lg_ssem,
    lg_rsem,
    in_sem,
    w_sem,
):
    me = lax.axis_index("tbl")
    px = lax.axis_index("pair")
    y = me // NZC
    zc = me % NZC
    z = zc // 2
    core = zc % 2

    sc_load = pltpu.make_async_copy(scales, sc_in, in_sem)
    sc_load.start()
    weights = ((w1, w1v), (b1, b1v), (w2, w2v), (b2, b2v), (w3, w3v), (b3, b3v), (w4, w4v), (b4, b4v))
    loads = [pltpu.make_async_copy(src, dst, w_sem.at[i]) for i, (src, dst) in enumerate(weights)]
    for load in loads:
        load.start()

    y_peers = [((y + k) % NY) for k in (1, 3, 2)]
    z_peers = [((z + dz) % 8) * 2 + c for dz in Z_ORDER for c in range(2)] + [z * 2 + (1 - core)]
    x_peers = [((px + k) % NX) for k in (1, 3, 2)]

    barrier = pltpu.get_barrier_semaphore()
    for peer in y_peers:
        pl.semaphore_signal(barrier, inc=1, device_id={"tbl": peer * NZC + zc}, device_id_type=MESH)
    for peer in z_peers:
        pl.semaphore_signal(barrier, inc=1, device_id={"tbl": y * NZC + peer}, device_id_type=MESH)
    for peer in x_peers:
        pl.semaphore_signal(barrier, inc=1, device_id={"pair": peer}, device_id_type=MESH)
    pl.semaphore_wait(barrier, len(y_peers) + len(z_peers) + len(x_peers))

    def send_y(ch):
        q = ch // NG
        g = ch % NG
        for peer in y_peers:
            pltpu.make_async_remote_copy(
                src_ref=codes.at[:, pl.ds(g * 2, 2), pl.ds(peer * NZC, NZC), q],
                dst_ref=y_recv.at[ch, y],
                send_sem=y_ssem.at[ch],
                recv_sem=y_rsem.at[ch],
                device_id={"tbl": peer * NZC + zc},
                device_id_type=MESH,
            ).start()
        pltpu.make_async_copy(
            codes.at[:, pl.ds(g * 2, 2), pl.ds(y * NZC, NZC), q], y_recv.at[ch, y], y_rsem.at[ch]
        ).start()

    send_y(0)

    sc_load.wait()
    sc_send[...] = sc_in[...].reshape(NY * 8, 16, 128).astype(BF16)
    y_sc[y] = sc_send[pl.ds(y * 8, 8)]
    for peer in y_peers:
        pltpu.make_async_remote_copy(
            src_ref=sc_send.at[pl.ds(peer * 8, 8)],
            dst_ref=y_sc.at[y],
            send_sem=sc_ssem.at[0],
            recv_sem=sc_rsem.at[0],
            device_id={"tbl": peer * NZC + zc},
            device_id_type=MESH,
        ).start()
    for ch in range(1, AHEAD):
        send_y(ch)

    for load in loads:
        load.wait()
    row = lax.broadcasted_iota(jnp.int32, (SHIFTS * 32, PAIRS), 0)
    col = lax.broadcasted_iota(jnp.int32, (SHIFTS * 32, PAIRS), 1)
    first = row % 32
    second = first + row // 32 + 1
    second = jnp.where(second >= TABLES, second - TABLES, second)
    low = jnp.minimum(first, second)
    high = jnp.maximum(first, second)
    rank = low * TABLES - (low * (low + 1)) // 2 + high - low - 1
    chosen = jnp.where((rank == col) & (first < TABLES), 1.0, 0.0).astype(BF16)
    w1p[...] = jnp.dot(chosen, w1v[...], preferred_element_type=F32).astype(BF16)
    xt[...] = jnp.zeros_like(xt)
    acc[...] = jnp.zeros_like(acc)

    flags = [[slot_ref[((p * NZC) + zc) * 2 + j] for j in range(2)] for p in range(2)]

    def merge(ch):
        pltpu.make_async_copy(y_recv.at[ch], y_recv.at[ch], y_rsem.at[ch]).wait()
        for p in range(2):
            for j in range(2):
                take_low = flags[p][j] >= 0
                for g in range(2):
                    merged[ch, :, p, j, g] = jnp.where(take_low, y_recv[ch, p, j, g], y_recv[ch, p + 2, j, g])
        for peer in z_peers:
            pltpu.make_async_remote_copy(
                src_ref=merged.at[ch, peer],
                dst_ref=z_recv.at[ch, zc],
                send_sem=z_ssem.at[ch],
                recv_sem=z_rsem.at[ch],
                device_id={"tbl": y * NZC + peer},
                device_id_type=MESH,
            ).start()
        z_recv[ch, zc] = merged[ch, zc]

    def merge_scales():
        pltpu.make_async_copy(y_sc.at[pl.ds(0, 3)], y_sc.at[pl.ds(0, 3)], sc_rsem.at[0]).wait()
        odd = lax.broadcasted_iota(jnp.int32, (8, 16, 128), 1) % 2
        picked = []
        for p in range(2):
            mask = jnp.where(odd == 0, flags[p][0], flags[p][1]) >= 0
            picked.append(jnp.where(mask, y_sc[p].astype(F32), y_sc[p + 2].astype(F32)))
        for c in range(2):
            both = jnp.concatenate([part[:, c * 8 : c * 8 + 8] for part in picked], axis=1)
            m_sc[:, c] = both.astype(BF16)
        for peer in z_peers:
            pltpu.make_async_remote_copy(
                src_ref=m_sc.at[peer // 2, peer % 2],
                dst_ref=z_sc.at[zc],
                send_sem=sc_ssem.at[1],
                recv_sem=sc_rsem.at[1],
                device_id={"tbl": y * NZC + peer},
                device_id_type=MESH,
            ).start()
        z_sc[zc] = m_sc[z, core]

    def spread_scales():
        pltpu.make_async_copy(z_sc.at[pl.ds(0, NZC - 1)], z_sc.at[pl.ds(0, NZC - 1)], sc_rsem.at[1]).wait()

        def body(s, carry):
            rows = z_sc[s].astype(F32)
            for p in range(2):
                for q in range(NQ):
                    for j in range(2):
                        r = p * 8 + q * 2 + j
                        sc[q * 64 + s * 4 + p * 2 + j] = jnp.broadcast_to(rows[r : r + 1], (8, 128))
            return carry

        lax.fori_loop(0, NZC, body, 0)

    def gram(ch):
        q = ch // NG
        pltpu.make_async_copy(z_recv.at[ch, pl.ds(0, NZC - 1)], z_recv.at[ch, pl.ds(0, NZC - 1)], z_rsem.at[ch]).wait()

        def widen(s, carry):
            unit[pl.ds(s * 4, 4)] = z_recv[ch, s].reshape(4, 2, 8, 128).astype(F32)
            return carry

        lax.fori_loop(0, NZC, widen, 0)

        def place(t, carry, again):
            for h in range(2):
                at = place_ref[t * 2 + h]
                factor = sc[q * 64 + at]
                both = unit[at]
                for g in range(2):
                    value = both[g] * factor
                    vals[h * 2 + g, t] = value
                    if again:
                        vals[h * 2 + g, t + TABLES] = value
            return carry

        lax.fori_loop(0, SHIFTS, functools.partial(place, again=True), 0)
        lax.fori_loop(SHIFTS, TABLES, functools.partial(place, again=False), 0)

        def shift(d, carry):
            for b in range(0, TABLES, 9):
                total = acc[d, b : b + 9]
                for k in range(4):
                    total = total + vals[k, b : b + 9] * vals[k, pl.ds(d + 1 + b, 9)]
                acc[d, b : b + 9] = total
            return carry

        lax.fori_loop(0, SHIFTS, shift, 0)

    def layer(inputs, weight, bias):
        product = jnp.dot(inputs, weight[...], preferred_element_type=F32)
        return jnp.maximum(product + bias[...], 0.0).astype(BF16)

    def finish(q):
        def fold(d, carry):
            xt[pl.ds(pl.multiple_of(d * 32, 32), TABLES)] = jnp.sum(acc[d], axis=1)
            acc[d] = jnp.zeros((TABLES, 8, 128), F32)
            return carry

        lax.fori_loop(0, SHIFTS, fold, 0)
        hidden = xt[...].T.astype(BF16)
        hidden = layer(hidden, w1p, b1v)
        hidden = layer(hidden, w2v, b2v)
        hidden = layer(hidden, w3v, b3v)
        hidden = layer(hidden, w4v, b4v)
        last = jnp.broadcast_to(wout_ref[...].astype(F32), (8, 256)).astype(BF16)
        final = lax.dot_general(last, hidden, (((1,), (1,)), ((), ())), preferred_element_type=F32)
        lg[px, q] = final + bout_ref[0]
        for peer in x_peers:
            pltpu.make_async_remote_copy(
                src_ref=lg.at[px, q],
                dst_ref=lg.at[px, q],
                send_sem=lg_ssem.at[q],
                recv_sem=lg_rsem.at[q],
                device_id={"pair": peer},
                device_id_type=MESH,
            ).start()

    def step(i, carry):
        @pl.when(i < CHUNKS)
        def _():
            merge(i)

        @pl.when(i + AHEAD < CHUNKS)
        def _():
            send_y(i + AHEAD)

        @pl.when(i == 0)
        def _():
            merge_scales()

        @pl.when(i == LAG)
        def _():
            spread_scales()

        @pl.when(i >= LAG)
        def _():
            gram(i - LAG)

        @pl.when((i >= LAG) & ((i - LAG) % NG == NG - 1))
        def _():
            finish((i - LAG) // NG)

        return carry

    lax.fori_loop(0, CHUNKS + LAG, step, 0)

    def sent(ch, carry):
        three = y_recv.at[ch, pl.ds(0, 3)]
        pltpu.make_async_copy(three, three, y_ssem.at[ch]).wait()
        most = z_recv.at[ch, pl.ds(0, NZC - 1)]
        pltpu.make_async_copy(most, most, z_ssem.at[ch]).wait()
        return carry

    lax.fori_loop(0, CHUNKS, sent, 0)
    pltpu.make_async_copy(y_sc.at[pl.ds(0, 3)], y_sc.at[pl.ds(0, 3)], sc_ssem.at[0]).wait()
    pltpu.make_async_copy(z_sc.at[pl.ds(0, NZC - 1)], z_sc.at[pl.ds(0, NZC - 1)], sc_ssem.at[1]).wait()
    for q in range(NQ):
        three = lg.at[pl.ds(0, 3), q]
        pltpu.make_async_copy(three, three, lg_ssem.at[q]).wait()
        pltpu.make_async_copy(three, three, lg_rsem.at[q]).wait()
    for p in range(NX):
        for q in range(NQ):
            out_ref[p : p + 1, q * 128 : (q + 1) * 128] = lg[p, q, 0:1]


def per_device(codes, scales, shard_slot, w1, b1, w2, b2, w3, b3, w4, b4, wout, bout):
    flat = shard_slot.reshape(-1)
    spot = jnp.arange(flat.shape[0], dtype=jnp.int32)
    half = flat.shape[0] // 2
    merged_spot = spot % half
    row, j = merged_spot // 2, merged_spot % 2
    merged_spot = (row % NZC) * 4 + (row // NZC) * 2 + j
    matches = flat[None, :] == jnp.arange(2 * TABLES, dtype=jnp.int32)[:, None]
    place = jnp.sum(jnp.where(matches, merged_spot[None, :], 0), axis=1).astype(jnp.int32)

    codes = codes.reshape(2, 8, 8, NY * NZC, NQ, 128).transpose(0, 1, 3, 4, 2, 5)
    scales = scales.reshape(2, NY * NZC, NQ, 128).transpose(1, 2, 0, 3).reshape(NY * NZC, 8, 128)

    any_spec = pl.BlockSpec(memory_space=pl.ANY)
    smem = pl.BlockSpec(memory_space=pltpu.SMEM)
    vmem = pl.BlockSpec(memory_space=pltpu.VMEM)
    dma = pltpu.SemaphoreType.DMA
    return pl.pallas_call(
        kernel,
        out_shape=jax.ShapeDtypeStruct((NX, NQ * 128), F32),
        in_specs=[smem, smem, smem] + [any_spec] * 10 + [vmem],
        out_specs=vmem,
        scratch_shapes=[
            pltpu.VMEM((CHUNKS, NY, 2, 2, NZC, 8, 128), BF16),
            pltpu.VMEM((CHUNKS, NZC, 2, 2, 2, 8, 128), BF16),
            pltpu.VMEM((CHUNKS, NZC, 2, 2, 2, 8, 128), BF16),
            pltpu.VMEM((NY * NZC, 8, 128), F32),
            pltpu.VMEM((NY * 8, 16, 128), BF16),
            pltpu.VMEM((NY, 8, 16, 128), BF16),
            pltpu.VMEM((8, 2, 16, 128), BF16),
            pltpu.VMEM((NZC, 16, 128), BF16),
            pltpu.VMEM((NQ * 64, 8, 128), F32),
            pltpu.VMEM((64, 2, 8, 128), F32),
            pltpu.VMEM((4, TABLES + SHIFTS, 8, 128), F32),
            pltpu.VMEM((SHIFTS, TABLES, 8, 128), F32),
            pltpu.VMEM((SHIFTS * 32, 128), F32),
            pltpu.VMEM((NX, NQ, 8, 128), F32),
            pltpu.VMEM(w1.shape, BF16),
            pltpu.VMEM((SHIFTS * 32, w1.shape[1]), BF16),
            pltpu.VMEM((1, b1.shape[0]), F32),
            pltpu.VMEM(w2.shape, BF16),
            pltpu.VMEM((1, b2.shape[0]), F32),
            pltpu.VMEM(w3.shape, BF16),
            pltpu.VMEM((1, b3.shape[0]), F32),
            pltpu.VMEM(w4.shape, BF16),
            pltpu.VMEM((1, b4.shape[0]), F32),
            dma((CHUNKS,)),
            dma((CHUNKS,)),
            dma((CHUNKS,)),
            dma((CHUNKS,)),
            dma((2,)),
            dma((2,)),
            dma((NQ,)),
            dma((NQ,)),
            dma,
            dma((8,)),
        ],
        compiler_params=pltpu.CompilerParams(
            collective_id=0, has_side_effects=True, vmem_limit_bytes=56 * 1024 * 1024
        ),
    )(flat, place, bout, codes, scales, w1, b1[None], w2, b2[None], w3, b3[None], w4, b4[None], wout[None])


def solution(mesh):
    return jax.shard_map(
        per_device,
        mesh=mesh,
        in_specs=(P("tbl", None, "pair"), P("tbl", "pair")) + (P(),) * 11,
        out_specs=P(None, "tbl"),
        check_vma=False,
    )
```

```python
import functools

import jax
import jax.numpy as jnp
from jax import lax
from jax.experimental import pallas as pl
from jax.experimental.pallas import tpu as pltpu
from jax.sharding import PartitionSpec as P

MESH = pl.DeviceIdType.MESH
F32 = jnp.float32
BF16 = jnp.bfloat16

TABLES = 27
SHIFTS = TABLES // 2
PAIRS = TABLES * SHIFTS
NY, NZC, NX = 4, 16, 4
NQ, NG = 4, 8
SPLIT = 1
J = 2 // SPLIT
CHUNKS = NQ * NG * SPLIT
AHEAD = 6 * SPLIT
LAG = 4 * SPLIT - 1
Z_ORDER = (4, 3, 5, 2, 6, 1, 7)


def kernel(
    slots,
    codes,
    scales,
    w1,
    b1,
    w2,
    b2,
    w3,
    b3,
    w4,
    b4,
    wout,
    out_ref,
    slot_v,
    slot_s,
    place_v,
    place_s,
    woutv,
    y_recv,
    merged,
    z_recv,
    sc_in,
    sc_send,
    y_sc,
    m_sc,
    z_sc,
    sc,
    unit,
    vals,
    acc,
    xt,
    lg,
    w1v,
    w1p,
    b1v,
    w2v,
    b2v,
    w3v,
    b3v,
    w4v,
    b4v,
    y_ssem,
    y_rsem,
    z_ssem,
    z_rsem,
    sc_ssem,
    sc_rsem,
    lg_ssem,
    lg_rsem,
    in_sem,
    slot_sem,
    w_sem,
):
    me = lax.axis_index("tbl")
    px = lax.axis_index("pair")
    y = me // NZC
    zc = me % NZC
    z = zc // 2
    core = zc % 2

    sc_load = pltpu.make_async_copy(scales, sc_in, in_sem)
    sc_load.start()
    slot_loads = [
        pltpu.make_async_copy(slots, slot_v, slot_sem.at[0]),
        pltpu.make_async_copy(slots, slot_s, slot_sem.at[1]),
    ]
    for load in slot_loads:
        load.start()
    weights = ((w1, w1v), (b1, b1v), (w2, w2v), (b2, b2v), (w3, w3v), (b3, b3v), (w4, w4v), (b4, b4v), (wout, woutv))
    loads = [pltpu.make_async_copy(src, dst, w_sem.at[i]) for i, (src, dst) in enumerate(weights)]
    for load in loads:
        load.start()

    y_peers = [((y + k) % NY) for k in (1, 3, 2)]
    z_peers = [((z + dz) % 8) * 2 + c for dz in Z_ORDER for c in range(2)] + [z * 2 + (1 - core)]
    x_peers = [((px + k) % NX) for k in (1, 3, 2)]

    barrier = pltpu.get_barrier_semaphore()
    for peer in y_peers:
        pl.semaphore_signal(barrier, inc=1, device_id={"tbl": peer * NZC + zc}, device_id_type=MESH)
    for peer in z_peers:
        pl.semaphore_signal(barrier, inc=1, device_id={"tbl": y * NZC + peer}, device_id_type=MESH)
    for peer in x_peers:
        pl.semaphore_signal(barrier, inc=1, device_id={"pair": peer}, device_id_type=MESH)
    pl.semaphore_wait(barrier, len(y_peers) + len(z_peers) + len(x_peers))

    def send_y(ch):
        q = ch // (NG * SPLIT)
        g = ch // SPLIT % NG
        j = ch % SPLIT
        for peer in y_peers:
            pltpu.make_async_remote_copy(
                src_ref=codes.at[pl.ds(j, J), g, pl.ds(peer * NZC, NZC), q],
                dst_ref=y_recv.at[ch, y],
                send_sem=y_ssem.at[ch],
                recv_sem=y_rsem.at[ch],
                device_id={"tbl": peer * NZC + zc},
                device_id_type=MESH,
            ).start()
        pltpu.make_async_copy(
            codes.at[pl.ds(j, J), g, pl.ds(y * NZC, NZC), q], y_recv.at[ch, y], y_rsem.at[ch]
        ).start()

    send_y(0)

    sc_load.wait()
    sc_send[...] = sc_in[...].reshape(NY * 8, 16, 128).astype(BF16)
    y_sc[y] = sc_send[pl.ds(y * 8, 8)]
    for peer in y_peers:
        pltpu.make_async_remote_copy(
            src_ref=sc_send.at[pl.ds(peer * 8, 8)],
            dst_ref=y_sc.at[y],
            send_sem=sc_ssem.at[0],
            recv_sem=sc_rsem.at[0],
            device_id={"tbl": peer * NZC + zc},
            device_id_type=MESH,
        ).start()
    for ch in range(1, AHEAD):
        send_y(ch)

    for load in loads:
        load.wait()
    row = lax.broadcasted_iota(jnp.int32, (SHIFTS * 32, PAIRS), 0)
    col = lax.broadcasted_iota(jnp.int32, (SHIFTS * 32, PAIRS), 1)
    first = row % 32
    second = first + row // 32 + 1
    second = jnp.where(second >= TABLES, second - TABLES, second)
    low = jnp.minimum(first, second)
    high = jnp.maximum(first, second)
    rank = low * TABLES - (low * (low + 1)) // 2 + high - low - 1
    chosen = jnp.where((rank == col) & (first < TABLES), 1.0, 0.0).astype(BF16)
    w1p[...] = jnp.dot(chosen, w1v[...], preferred_element_type=F32).astype(BF16)
    xt[...] = jnp.zeros_like(xt)
    acc[...] = jnp.zeros_like(acc)

    for load in slot_loads:
        load.wait()
    shard = lax.broadcasted_iota(jnp.int32, (56, NY * NZC), 0)
    table_row = lax.broadcasted_iota(jnp.int32, (56, NY * NZC), 1) % (2 * NZC)
    spot = table_row % NZC * 4 + table_row // NZC * 2
    place = jnp.zeros((56, 1), jnp.int32)
    for j in range(2):
        here = jnp.broadcast_to(slot_v[j : j + 1], shard.shape) == shard
        found = jnp.max(jnp.where(here, spot + j, 0), axis=1, keepdims=True)
        place = jnp.maximum(place, found)
    place_v[...] = jnp.broadcast_to(place, (56, 128))
    place_copy = pltpu.make_async_copy(place_v, place_s, slot_sem.at[0])
    place_copy.start()
    place_copy.wait()
    flags = [[slot_s[j, p * NZC + zc] for j in range(2)] for p in range(2)]

    def merge(ch):
        pltpu.make_async_copy(y_recv.at[ch], y_recv.at[ch], y_rsem.at[ch]).wait()
        for p in range(2):
            for n in range(J):
                flag = flags[p][n] if SPLIT == 1 else jnp.where(ch % 2 == 0, flags[p][0], flags[p][1])
                merged[ch, :, p, n] = jnp.where(flag >= 0, y_recv[ch, p, n], y_recv[ch, p + 2, n])
        for peer in z_peers:
            pltpu.make_async_remote_copy(
                src_ref=merged.at[ch, peer],
                dst_ref=z_recv.at[ch, zc],
                send_sem=z_ssem.at[ch],
                recv_sem=z_rsem.at[ch],
                device_id={"tbl": y * NZC + peer},
                device_id_type=MESH,
            ).start()
        z_recv[ch, zc] = merged[ch, zc]

    def merge_scales():
        pltpu.make_async_copy(y_sc.at[pl.ds(0, 3)], y_sc.at[pl.ds(0, 3)], sc_rsem.at[0]).wait()
        odd = lax.broadcasted_iota(jnp.int32, (8, 16, 128), 1) % 2
        picked = []
        for p in range(2):
            mask = jnp.where(odd == 0, flags[p][0], flags[p][1]) >= 0
            picked.append(jnp.where(mask, y_sc[p].astype(F32), y_sc[p + 2].astype(F32)))
        for c in range(2):
            both = jnp.concatenate([part[:, c * 8 : c * 8 + 8] for part in picked], axis=1)
            m_sc[:, c] = both.astype(BF16)
        for peer in z_peers:
            pltpu.make_async_remote_copy(
                src_ref=m_sc.at[peer // 2, peer % 2],
                dst_ref=z_sc.at[zc],
                send_sem=sc_ssem.at[1],
                recv_sem=sc_rsem.at[1],
                device_id={"tbl": y * NZC + peer},
                device_id_type=MESH,
            ).start()
        z_sc[zc] = m_sc[z, core]

    def spread_scales():
        pltpu.make_async_copy(z_sc.at[pl.ds(0, NZC - 1)], z_sc.at[pl.ds(0, NZC - 1)], sc_rsem.at[1]).wait()

        def body(s, carry):
            rows = z_sc[s].astype(F32)
            for p in range(2):
                for q in range(NQ):
                    for j in range(2):
                        r = p * 8 + q * 2 + j
                        sc[q * 64 + s * 4 + p * 2 + j] = jnp.broadcast_to(rows[r : r + 1], (8, 128))
            return carry

        lax.fori_loop(0, NZC, body, 0)

    def gram(n):
        q = n // NG
        for part in range(SPLIT):
            most = z_recv.at[n * SPLIT + part, pl.ds(0, NZC - 1)]
            pltpu.make_async_copy(most, most, z_rsem.at[n * SPLIT + part]).wait()

        def widen(s, carry):
            for half in range(2):
                for p in range(2):
                    for j in range(2):
                        chunk = n if SPLIT == 1 else n * 2 + j
                        piece = z_recv[chunk, s * 2 + half, p, j if SPLIT == 1 else 0]
                        unit[s * 8 + half * 4 + p * 2 + j] = piece.astype(F32)
            return carry

        lax.fori_loop(0, NZC // 2, widen, 0)

        def place_three(b, carry):
            for r in range(3):
                t = b * 3 + r
                for h in range(2):
                    at = place_s[t * 2 + h, 0]
                    vals[h, t] = unit[at] * sc[q * 64 + at]
            return carry

        lax.fori_loop(0, TABLES // 3, place_three, 0)
        for h in range(2):
            vals[h, TABLES : TABLES + SHIFTS + 1] = vals[h, 0 : SHIFTS + 1]

        def shift(e, carry):
            d = e * 2
            for b in range(0, TABLES, 9):
                one = acc[d, b : b + 9]
                two = acc[d + 1, b : b + 9]
                for h in range(2):
                    left = vals[h, b : b + 9]
                    right = vals[h, pl.ds(d + 1 + b, 10)]
                    one = one + left * right[0:9]
                    two = two + left * right[1:10]
                acc[d, b : b + 9] = one
                acc[d + 1, b : b + 9] = two
            return carry

        lax.fori_loop(0, (SHIFTS + 1) // 2, shift, 0)

    def layer(inputs, weight, bias):
        product = jnp.dot(inputs, weight[...], preferred_element_type=F32)
        return jnp.maximum(product + bias[...], 0.0).astype(BF16)

    def finish(q):
        def fold(d, carry):
            xt[pl.ds(pl.multiple_of(d * 32, 32), TABLES)] = jnp.sum(acc[d], axis=1)
            acc[d] = jnp.zeros((TABLES, 8, 128), F32)
            return carry

        lax.fori_loop(0, SHIFTS, fold, 0)
        hidden = xt[...].T.astype(BF16)
        hidden = layer(hidden, w1p, b1v)
        hidden = layer(hidden, w2v, b2v)
        hidden = layer(hidden, w3v, b3v)
        hidden = layer(hidden, w4v, b4v)
        last = jnp.broadcast_to(woutv[...].astype(F32).reshape(1, 256), (8, 256)).astype(BF16)
        final = lax.dot_general(last, hidden, (((1,), (1,)), ((), ())), preferred_element_type=F32)
        lg[px, q] = final
        for peer in x_peers:
            pltpu.make_async_remote_copy(
                src_ref=lg.at[px, q],
                dst_ref=lg.at[px, q],
                send_sem=lg_ssem.at[q],
                recv_sem=lg_rsem.at[q],
                device_id={"pair": peer},
                device_id_type=MESH,
            ).start()

    def step(i, carry):
        @pl.when(i < CHUNKS)
        def _():
            merge(i)

        @pl.when(i + AHEAD < CHUNKS)
        def _():
            send_y(i + AHEAD)

        @pl.when(i == 0)
        def _():
            merge_scales()

        @pl.when(i == LAG)
        def _():
            spread_scales()

        @pl.when((i >= LAG) & ((i - LAG) % SPLIT == 0))
        def _():
            gram((i - LAG) // SPLIT)

        @pl.when((i >= LAG) & ((i - LAG) % (NG * SPLIT) == (NG - 1) * SPLIT))
        def _():
            finish((i - LAG) // (NG * SPLIT))

        return carry

    lax.fori_loop(0, CHUNKS + LAG - SPLIT + 1, step, 0)

    def sent(ch, carry):
        three = y_recv.at[ch, pl.ds(0, 3)]
        pltpu.make_async_copy(three, three, y_ssem.at[ch]).wait()
        most = z_recv.at[ch, pl.ds(0, NZC - 1)]
        pltpu.make_async_copy(most, most, z_ssem.at[ch]).wait()
        return carry

    lax.fori_loop(0, CHUNKS, sent, 0)
    pltpu.make_async_copy(y_sc.at[pl.ds(0, 3)], y_sc.at[pl.ds(0, 3)], sc_ssem.at[0]).wait()
    pltpu.make_async_copy(z_sc.at[pl.ds(0, NZC - 1)], z_sc.at[pl.ds(0, NZC - 1)], sc_ssem.at[1]).wait()
    for q in range(NQ):
        three = lg.at[pl.ds(0, 3), q]
        pltpu.make_async_copy(three, three, lg_ssem.at[q]).wait()
        pltpu.make_async_copy(three, three, lg_rsem.at[q]).wait()
    for p in range(NX):
        for q in range(NQ):
            out_ref[p : p + 1, q * 128 : (q + 1) * 128] = lg[p, q, 0:1]


def per_device(codes, scales, shard_slot, w1, b1, w2, b2, w3, b3, w4, b4, wout, bout):
    codes = codes.reshape(2, 8, 8, NY * NZC, NQ, 128).transpose(0, 1, 3, 4, 2, 5)
    scales = scales.reshape(2, NY * NZC, NQ, 128).transpose(1, 2, 0, 3).reshape(NY * NZC, 8, 128)

    any_spec = pl.BlockSpec(memory_space=pl.ANY)
    vmem = pl.BlockSpec(memory_space=pltpu.VMEM)
    dma = pltpu.SemaphoreType.DMA
    logits = pl.pallas_call(
        kernel,
        out_shape=jax.ShapeDtypeStruct((NX, NQ * 128), F32),
        in_specs=[any_spec] * 12,
        out_specs=vmem,
        scratch_shapes=[
            pltpu.VMEM((2, NY * NZC), jnp.int32),
            pltpu.SMEM((2, NY * NZC), jnp.int32),
            pltpu.VMEM((56, 128), jnp.int32),
            pltpu.SMEM((56, 128), jnp.int32),
            pltpu.VMEM(wout.shape, BF16),
            pltpu.VMEM((CHUNKS, NY, J, NZC, 8, 128), BF16),
            pltpu.VMEM((CHUNKS, NZC, 2, J, 8, 128), BF16),
            pltpu.VMEM((CHUNKS, NZC, 2, J, 8, 128), BF16),
            pltpu.VMEM((NY * NZC, 8, 128), F32),
            pltpu.VMEM((NY * 8, 16, 128), BF16),
            pltpu.VMEM((NY, 8, 16, 128), BF16),
            pltpu.VMEM((8, 2, 16, 128), BF16),
            pltpu.VMEM((NZC, 16, 128), BF16),
            pltpu.VMEM((NQ * 64, 8, 128), F32),
            pltpu.VMEM((64, 8, 128), F32),
            pltpu.VMEM((2, TABLES + SHIFTS + 1, 8, 128), F32),
            pltpu.VMEM((SHIFTS + 1, TABLES, 8, 128), F32),
            pltpu.VMEM((SHIFTS * 32, 128), F32),
            pltpu.VMEM((NX, NQ, 8, 128), F32),
            pltpu.VMEM(w1.shape, BF16),
            pltpu.VMEM((SHIFTS * 32, w1.shape[1]), BF16),
            pltpu.VMEM((1, b1.shape[0]), F32),
            pltpu.VMEM(w2.shape, BF16),
            pltpu.VMEM((1, b2.shape[0]), F32),
            pltpu.VMEM(w3.shape, BF16),
            pltpu.VMEM((1, b3.shape[0]), F32),
            pltpu.VMEM(w4.shape, BF16),
            pltpu.VMEM((1, b4.shape[0]), F32),
            dma((CHUNKS,)),
            dma((CHUNKS,)),
            dma((CHUNKS,)),
            dma((CHUNKS,)),
            dma((2,)),
            dma((2,)),
            dma((NQ,)),
            dma((NQ,)),
            dma,
            dma((2,)),
            dma((9,)),
        ],
        compiler_params=pltpu.CompilerParams(
            collective_id=0, has_side_effects=True, vmem_limit_bytes=56 * 1024 * 1024
        ),
    )(shard_slot.T, codes, scales, w1, b1[None], w2, b2[None], w3, b3[None], w4, b4[None], wout)
    return logits + bout


def solution(mesh):
    return jax.shard_map(
        per_device,
        mesh=mesh,
        in_specs=(P("tbl", None, "pair"), P("tbl", "pair")) + (P(),) * 11,
        out_specs=P(None, "tbl"),
        check_vma=False,
    )
```

```python
import functools

import jax
import jax.numpy as jnp
from jax import lax
from jax.experimental import pallas as pl
from jax.experimental.pallas import tpu as pltpu
from jax.sharding import PartitionSpec as P

MESH = pl.DeviceIdType.MESH
F32 = jnp.float32
BF16 = jnp.bfloat16

TABLES = 27
SHIFTS = TABLES // 2
PAIRS = TABLES * SHIFTS
NY, NZC, NX = 4, 16, 4
NQ, NG = 4, 8
GROUPS = NQ * NG
CHUNKS = GROUPS - 1
AHEAD = 6
LAG = 3
Z_ORDER = (4, 3, 5, 2, 6, 1, 7)


def kernel(
    slots,
    codes,
    scales,
    w1,
    b1,
    w2,
    b2,
    w3,
    b3,
    w4,
    b4,
    wout,
    out_ref,
    slot_v,
    slot_s,
    place_v,
    place_s,
    woutv,
    y_recv,
    merged,
    z_recv,
    early,
    late,
    sc_in,
    rows,
    unit,
    vals,
    acc,
    xt,
    lg,
    w1v,
    w1p,
    b1v,
    w2v,
    b2v,
    w3v,
    b3v,
    w4v,
    b4v,
    y_ssem,
    y_rsem,
    z_ssem,
    z_rsem,
    row_sem,
    lg_ssem,
    lg_rsem,
    own_sem,
    side_sem,
    in_sem,
    slot_sem,
    w_sem,
):
    me = lax.axis_index("tbl")
    px = lax.axis_index("pair")
    y = me // NZC
    zc = me % NZC
    z = zc // 2
    core = zc % 2

    y_peers = [((y + k) % NY) for k in (1, 3, 2)]
    z_peers = [((z + dz) % 8) * 2 + c for dz in Z_ORDER for c in range(2)] + [z * 2 + (1 - core)]
    x_peers = [((px + k) % NX) for k in (1, 3, 2)]

    barrier = pltpu.get_barrier_semaphore()
    for peer in y_peers:
        pl.semaphore_signal(barrier, inc=1, device_id={"tbl": peer * NZC + zc}, device_id_type=MESH)
    for peer in z_peers:
        pl.semaphore_signal(barrier, inc=1, device_id={"tbl": y * NZC + peer}, device_id_type=MESH)
    for peer in x_peers:
        pl.semaphore_signal(barrier, inc=1, device_id={"pair": peer}, device_id_type=MESH)

    sc_load = pltpu.make_async_copy(scales, sc_in, in_sem)
    sc_load.start()

    def load_rows(n):
        return pltpu.make_async_copy(codes.at[:, n % NG, :, :, n // NG], rows.at[n], row_sem.at[n])

    load_rows(0).start()
    load_rows(CHUNKS).start()
    slot_loads = [
        pltpu.make_async_copy(slots, slot_v, slot_sem.at[0]),
        pltpu.make_async_copy(slots, slot_s, slot_sem.at[1]),
    ]
    for load in slot_loads:
        load.start()
    weights = ((w1, w1v), (b1, b1v), (w2, w2v), (b2, b2v), (w3, w3v), (b3, b3v), (w4, w4v), (b4, b4v), (wout, woutv))
    loads = [pltpu.make_async_copy(src, dst, w_sem.at[i]) for i, (src, dst) in enumerate(weights)]
    lax.fori_loop(1, AHEAD + 2, lambda n, carry: (load_rows(n).start(), carry)[1], 0)
    for load in loads:
        load.start()


    def dequantize(n):
        load_rows(n).wait()
        q = n // NG

        def body(k, carry):
            for j in range(2):
                factor = sc_in[pl.ds(k * NZC, NZC), pl.ds(q * 2 + j, 1)]
                rows[n, j, k] = (rows[n, j, k].astype(F32) * factor).astype(BF16)
            return carry

        lax.fori_loop(0, NY, body, 0)

        @pl.when(n < CHUNKS)
        def _():
            y_recv[n, y] = rows[n, :, y]

    sc_load.wait()
    dequantize(0)
    pl.semaphore_wait(barrier, len(y_peers) + len(z_peers) + len(x_peers))

    def send_y(ch):
        for peer in y_peers:
            pltpu.make_async_remote_copy(
                src_ref=rows.at[ch, :, peer],
                dst_ref=y_recv.at[ch, y],
                send_sem=y_ssem.at[ch],
                recv_sem=y_rsem.at[ch],
                device_id={"tbl": peer * NZC + zc},
                device_id_type=MESH,
            ).start()

    send_y(0)
    dequantize(CHUNKS)

    for peer in z_peers:
        pltpu.make_async_remote_copy(
            src_ref=rows.at[CHUNKS, :, :, peer],
            dst_ref=early.at[zc],
            send_sem=side_sem.at[0],
            recv_sem=side_sem.at[1],
            device_id={"tbl": y * NZC + peer},
            device_id_type=MESH,
        ).start()
    early[zc] = rows[CHUNKS, :, :, zc]

    def send_late():
        pltpu.make_async_copy(early.at[pl.ds(0, NZC - 1)], early.at[pl.ds(0, NZC - 1)], side_sem.at[1]).wait()
        for peer in y_peers:
            pltpu.make_async_remote_copy(
                src_ref=early.at[:, :, peer],
                dst_ref=late.at[y],
                send_sem=side_sem.at[2],
                recv_sem=side_sem.at[3],
                device_id={"tbl": peer * NZC + zc},
                device_id_type=MESH,
            ).start()
        late[y] = early[:, :, y]


    for ch in range(1, AHEAD):
        dequantize(ch)
        send_y(ch)
    lax.fori_loop(AHEAD + 2, CHUNKS, lambda n, carry: (load_rows(n).start(), carry)[1], 0)
    dequantize(AHEAD)

    for load in loads:
        load.wait()
    row = lax.broadcasted_iota(jnp.int32, (SHIFTS * 32, PAIRS), 0)
    col = lax.broadcasted_iota(jnp.int32, (SHIFTS * 32, PAIRS), 1)
    first = row % 32
    second = first + row // 32 + 1
    second = jnp.where(second >= TABLES, second - TABLES, second)
    low = jnp.minimum(first, second)
    high = jnp.maximum(first, second)
    rank = low * TABLES - (low * (low + 1)) // 2 + high - low - 1
    chosen = jnp.where((rank == col) & (first < TABLES), 1.0, 0.0).astype(BF16)
    w1p[...] = jnp.dot(chosen, w1v[...], preferred_element_type=F32).astype(BF16)
    xt[...] = jnp.zeros_like(xt)
    acc[...] = jnp.zeros_like(acc)

    for load in slot_loads:
        load.wait()
    shard = lax.broadcasted_iota(jnp.int32, (56, NY * NZC), 0)
    table_row = lax.broadcasted_iota(jnp.int32, (56, NY * NZC), 1) % (2 * NZC)
    spot = table_row % NZC * 4 + table_row // NZC * 2
    place = jnp.zeros((56, 1), jnp.int32)
    for j in range(2):
        here = jnp.broadcast_to(slot_v[j : j + 1], shard.shape) == shard
        found = jnp.max(jnp.where(here, spot + j, 0), axis=1, keepdims=True)
        place = jnp.maximum(place, found)
    place_v[...] = jnp.broadcast_to(place, (56, 128))
    place_copy = pltpu.make_async_copy(place_v, place_s, slot_sem.at[0])
    place_copy.start()
    place_copy.wait()
    flags = [[slot_s[j, p * NZC + zc] for j in range(2)] for p in range(2)]

    def merge(ch):
        three = y_recv.at[ch, pl.ds(0, 3)]
        pltpu.make_async_copy(three, three, y_rsem.at[ch]).wait()
        for p in range(2):
            for j in range(2):
                merged[ch, :, p, j] = jnp.where(flags[p][j] >= 0, y_recv[ch, p, j], y_recv[ch, p + 2, j])
        for peer in z_peers:
            pltpu.make_async_remote_copy(
                src_ref=merged.at[ch, peer],
                dst_ref=z_recv.at[ch, zc],
                send_sem=z_ssem.at[ch],
                recv_sem=z_rsem.at[ch],
                device_id={"tbl": y * NZC + peer},
                device_id_type=MESH,
            ).start()
        z_recv[ch, zc] = merged[ch, zc]

    def gram(n):
        @pl.when(n != CHUNKS - 1)
        def _():
            ch = jnp.minimum(n, CHUNKS - 1)
            most = z_recv.at[ch, pl.ds(0, NZC - 1)]
            pltpu.make_async_copy(most, most, z_rsem.at[ch]).wait()

            def widen(s, carry):
                for half in range(2):
                    for p in range(2):
                        for j in range(2):
                            unit[s * 8 + half * 4 + p * 2 + j] = z_recv[ch, s * 2 + half, p, j].astype(F32)
                return carry

            lax.fori_loop(0, NZC // 2, widen, 0)

        @pl.when(n == CHUNKS - 1)
        def _():
            pltpu.make_async_copy(late.at[pl.ds(0, 3)], late.at[pl.ds(0, 3)], side_sem.at[3]).wait()

            def pick(s, carry):
                for p in range(2):
                    for j in range(2):
                        take_low = slot_s[j, p * NZC + s] >= 0
                        unit[s * 4 + p * 2 + j] = jnp.where(take_low, late[p, s, j], late[p + 2, s, j]).astype(F32)
                return carry

            lax.fori_loop(0, NZC, pick, 0)

        def place_three(b, carry):
            for r in range(3):
                t = b * 3 + r
                for h in range(2):
                    at = place_s[t * 2 + h, 0]
                    vals[h, t] = unit[at]
            return carry

        lax.fori_loop(0, TABLES // 3, place_three, 0)
        for h in range(2):
            vals[h, TABLES : TABLES + SHIFTS + 1] = vals[h, 0 : SHIFTS + 1]

        def shift(e, carry):
            d = e * 2
            for b in range(0, TABLES, 9):
                one = acc[d, b : b + 9]
                two = acc[d + 1, b : b + 9]
                for h in range(2):
                    left = vals[h, b : b + 9]
                    right = vals[h, pl.ds(d + 1 + b, 10)]
                    one = one + left * right[0:9]
                    two = two + left * right[1:10]
                acc[d, b : b + 9] = one
                acc[d + 1, b : b + 9] = two
            return carry

        lax.fori_loop(0, (SHIFTS + 1) // 2, shift, 0)

    def layer(inputs, weight, bias):
        product = jnp.dot(inputs, weight[...], preferred_element_type=F32)
        return jnp.maximum(product + bias[...], 0.0).astype(BF16)

    sub = lax.broadcasted_iota(jnp.int32, (8, 128), 0)

    def fold_rows(rows):
        for dist in (4, 2, 1):
            low = (sub & dist) == 0
            merged_rows = []
            for a in range(dist):
                one, two = rows[a], rows[a + dist]
                if one is None:
                    merged_rows.append(None)
                    continue
                two = jnp.zeros_like(one) if two is None else two
                other = jnp.where(low, two, one)
                if dist == 4:
                    moved = pltpu.roll(other, 4, 0)
                else:
                    moved = jnp.where(low, pltpu.roll(other, 8 - dist, 0), pltpu.roll(other, dist, 0))
                merged_rows.append(jnp.where(low, one, two) + moved)
            rows = merged_rows
        return rows[0]

    def finish(q):
        def fold(d, carry):
            for b in range(0, 32, 8):
                rows = [acc[d, b + r] if b + r < TABLES else None for r in range(8)]
                xt[pl.ds(pl.multiple_of(d * 32 + b, 8), 8)] = fold_rows(rows)
            acc[d] = jnp.zeros((TABLES, 8, 128), F32)
            return carry

        lax.fori_loop(0, SHIFTS, fold, 0)
        hidden = xt[...].T.astype(BF16)
        hidden = layer(hidden, w1p, b1v)
        hidden = layer(hidden, w2v, b2v)
        hidden = layer(hidden, w3v, b3v)
        hidden = layer(hidden, w4v, b4v)
        last = jnp.broadcast_to(woutv[...].astype(F32).reshape(1, 256), (8, 256)).astype(BF16)
        final = lax.dot_general(last, hidden, (((1,), (1,)), ((), ())), preferred_element_type=F32)
        lg[q] = final[0:1]
        pltpu.make_async_copy(lg.at[q], out_ref.at[q, px], own_sem.at[q]).start()
        for peer in x_peers:
            pltpu.make_async_remote_copy(
                src_ref=lg.at[q],
                dst_ref=out_ref.at[q, px],
                send_sem=lg_ssem.at[q],
                recv_sem=lg_rsem.at[q],
                device_id={"pair": peer},
                device_id_type=MESH,
            ).start()

    def step(i, carry):
        @pl.when(i < CHUNKS)
        def _():
            merge(i)

        @pl.when(i + AHEAD < CHUNKS)
        def _():
            send_y(i + AHEAD)

        @pl.when(i + AHEAD + 1 < CHUNKS)
        def _():
            dequantize(i + AHEAD + 1)

        @pl.when(i + AHEAD == CHUNKS)
        def _():
            send_late()

        @pl.when(i >= LAG)
        def _():
            gram(i - LAG)

        @pl.when((i >= LAG) & ((i - LAG) % NG == NG - 1))
        def _():
            finish((i - LAG) // NG)

        return carry

    lax.fori_loop(0, GROUPS + LAG, step, 0)

    def sent(ch, carry):
        three = y_recv.at[ch, pl.ds(0, 3)]
        pltpu.make_async_copy(three, three, y_ssem.at[ch]).wait()
        most = z_recv.at[ch, pl.ds(0, NZC - 1)]
        pltpu.make_async_copy(most, most, z_ssem.at[ch]).wait()
        return carry

    lax.fori_loop(0, CHUNKS, sent, 0)
    pltpu.make_async_copy(early.at[pl.ds(0, NZC - 1)], early.at[pl.ds(0, NZC - 1)], side_sem.at[0]).wait()
    pltpu.make_async_copy(late.at[pl.ds(0, 3)], late.at[pl.ds(0, 3)], side_sem.at[2]).wait()
    for q in range(NQ):
        three = out_ref.at[q, pl.ds(0, 3)]
        pltpu.make_async_copy(three, three, lg_ssem.at[q]).wait()
        pltpu.make_async_copy(lg.at[q], out_ref.at[q, px], own_sem.at[q]).wait()
        pltpu.make_async_copy(three, three, lg_rsem.at[q]).wait()


def per_device(codes, scales, shard_slot, w1, b1, w2, b2, w3, b3, w4, b4, wout, bout):
    codes = codes.reshape(2, NG, 8, NY, NZC, NQ, 128).transpose(0, 1, 3, 4, 5, 2, 6)
    scales = scales.reshape(2, NY * NZC, NQ, 128).transpose(1, 2, 0, 3).reshape(NY * NZC, 8, 128)

    any_spec = pl.BlockSpec(memory_space=pl.ANY)
    dma = pltpu.SemaphoreType.DMA
    logits = pl.pallas_call(
        kernel,
        out_shape=jax.ShapeDtypeStruct((NQ, NX, 1, 128), F32),
        in_specs=[any_spec] * 12,
        out_specs=any_spec,
        scratch_shapes=[
            pltpu.VMEM((2, NY * NZC), jnp.int32),
            pltpu.SMEM((2, NY * NZC), jnp.int32),
            pltpu.VMEM((56, 128), jnp.int32),
            pltpu.SMEM((56, 128), jnp.int32),
            pltpu.VMEM(wout.shape, BF16),
            pltpu.VMEM((CHUNKS, NY, 2, NZC, 8, 128), BF16),
            pltpu.VMEM((CHUNKS, NZC, 2, 2, 8, 128), BF16),
            pltpu.VMEM((CHUNKS, NZC, 2, 2, 8, 128), BF16),
            pltpu.VMEM((NZC, 2, NY, 8, 128), BF16),
            pltpu.VMEM((NY, NZC, 2, 8, 128), BF16),
            pltpu.VMEM((NY * NZC, 8, 128), F32),
            pltpu.VMEM((GROUPS, 2, NY, NZC, 8, 128), BF16),
            pltpu.VMEM((64, 8, 128), F32),
            pltpu.VMEM((2, TABLES + SHIFTS + 1, 8, 128), F32),
            pltpu.VMEM((SHIFTS + 1, TABLES, 8, 128), F32),
            pltpu.VMEM((SHIFTS * 32, 128), F32),
            pltpu.VMEM((NQ, 1, 128), F32),
            pltpu.VMEM(w1.shape, BF16),
            pltpu.VMEM((SHIFTS * 32, w1.shape[1]), BF16),
            pltpu.VMEM((1, b1.shape[0]), F32),
            pltpu.VMEM(w2.shape, BF16),
            pltpu.VMEM((1, b2.shape[0]), F32),
            pltpu.VMEM(w3.shape, BF16),
            pltpu.VMEM((1, b3.shape[0]), F32),
            pltpu.VMEM(w4.shape, BF16),
            pltpu.VMEM((1, b4.shape[0]), F32),
            dma((CHUNKS,)),
            dma((CHUNKS,)),
            dma((CHUNKS,)),
            dma((CHUNKS,)),
            dma((GROUPS,)),
            dma((NQ,)),
            dma((NQ,)),
            dma((NQ,)),
            dma((4,)),
            dma,
            dma((2,)),
            dma((9,)),
        ],
        compiler_params=pltpu.CompilerParams(
            collective_id=0, has_side_effects=True, vmem_limit_bytes=56 * 1024 * 1024
        ),
    )(shard_slot.T, codes, scales, w1, b1[None], w2, b2[None], w3, b3[None], w4, b4[None], wout)
    return logits.transpose(1, 2, 0, 3).reshape(NX, NQ * 128) + bout


def solution(mesh):
    return jax.shard_map(
        per_device,
        mesh=mesh,
        in_specs=(P("tbl", None, "pair"), P("tbl", "pair")) + (P(),) * 11,
        out_specs=P(None, "tbl"),
        check_vma=False,
    )
```

```python
import functools

import jax
import jax.numpy as jnp
from jax import lax
from jax.experimental import pallas as pl
from jax.experimental.pallas import tpu as pltpu
from jax.sharding import PartitionSpec as P

MESH = pl.DeviceIdType.MESH
F32 = jnp.float32
BF16 = jnp.bfloat16

TABLES = 27
SHIFTS = TABLES // 2
PAIRS = TABLES * SHIFTS
NY, NZC, NX = 4, 16, 4
NQ, NG = 4, 8
GROUPS = NQ * NG
CHUNKS = GROUPS - 1
AHEAD = 6
LAG = 3
Z_ORDER = (4, 3, 5, 2, 6, 1, 7)


def kernel(
    slots,
    codes,
    scales,
    w1,
    b1,
    w2,
    b2,
    w3,
    b3,
    w4,
    b4,
    wout,
    out_ref,
    slot_v,
    slot_s,
    place_v,
    place_s,
    woutv,
    y_recv,
    merged,
    z_recv,
    early,
    late,
    sc_in,
    rows,
    unit,
    vals,
    acc,
    xt,
    lg,
    w1v,
    w1p,
    b1v,
    w2v,
    b2v,
    w3v,
    b3v,
    w4v,
    b4v,
    y_ssem,
    y_rsem,
    z_ssem,
    z_rsem,
    row_sem,
    lg_ssem,
    lg_rsem,
    side_sem,
    in_sem,
    slot_sem,
    w_sem,
):
    me = lax.axis_index("tbl")
    px = lax.axis_index("pair")
    y = me // NZC
    zc = me % NZC
    z = zc // 2
    core = zc % 2

    y_peers = [((y + k) % NY) for k in (1, 3, 2)]
    z_peers = [((z + dz) % 8) * 2 + c for dz in Z_ORDER for c in range(2)] + [z * 2 + (1 - core)]
    x_peers = [((px + k) % NX) for k in (1, 3, 2)]

    barrier = pltpu.get_barrier_semaphore()
    for peer in y_peers:
        pl.semaphore_signal(barrier, inc=1, device_id={"tbl": peer * NZC + zc}, device_id_type=MESH)
    for peer in z_peers:
        pl.semaphore_signal(barrier, inc=1, device_id={"tbl": y * NZC + peer}, device_id_type=MESH)
    for peer in x_peers:
        pl.semaphore_signal(barrier, inc=1, device_id={"pair": peer}, device_id_type=MESH)

    sc_load = pltpu.make_async_copy(scales, sc_in, in_sem)
    sc_load.start()

    def load_rows(n):
        return pltpu.make_async_copy(codes.at[:, n % NG, :, :, n // NG], rows.at[n], row_sem.at[n])

    load_rows(0).start()
    load_rows(CHUNKS).start()
    slot_loads = [
        pltpu.make_async_copy(slots, slot_v, slot_sem.at[0]),
        pltpu.make_async_copy(slots, slot_s, slot_sem.at[1]),
    ]
    for load in slot_loads:
        load.start()
    weights = ((w1, w1v), (b1, b1v), (w2, w2v), (b2, b2v), (w3, w3v), (b3, b3v), (w4, w4v), (b4, b4v), (wout, woutv))
    loads = [pltpu.make_async_copy(src, dst, w_sem.at[i]) for i, (src, dst) in enumerate(weights)]
    lax.fori_loop(1, AHEAD + 2, lambda n, carry: (load_rows(n).start(), carry)[1], 0)
    for load in loads:
        load.start()


    def dequantize(n):
        load_rows(n).wait()
        q = n // NG

        def body(k, carry):
            for j in range(2):
                factor = sc_in[pl.ds(k * NZC, NZC), pl.ds(q * 2 + j, 1)]
                rows[n, j, k] = (rows[n, j, k].astype(F32) * factor).astype(BF16)
            return carry

        lax.fori_loop(0, NY, body, 0)

        @pl.when(n < CHUNKS)
        def _():
            y_recv[n, y] = rows[n, :, y]

    sc_load.wait()
    dequantize(0)
    dequantize(CHUNKS)
    pl.semaphore_wait(barrier, len(y_peers) + len(z_peers) + len(x_peers))

    def send_y(ch):
        for peer in y_peers:
            pltpu.make_async_remote_copy(
                src_ref=rows.at[ch, :, peer],
                dst_ref=y_recv.at[ch, y],
                send_sem=y_ssem.at[ch],
                recv_sem=y_rsem.at[ch],
                device_id={"tbl": peer * NZC + zc},
                device_id_type=MESH,
            ).start()

    send_y(0)

    for peer in z_peers:
        pltpu.make_async_remote_copy(
            src_ref=rows.at[CHUNKS, :, :, peer],
            dst_ref=early.at[zc],
            send_sem=side_sem.at[0],
            recv_sem=side_sem.at[1],
            device_id={"tbl": y * NZC + peer},
            device_id_type=MESH,
        ).start()
    early[zc] = rows[CHUNKS, :, :, zc]

    def send_late():
        pltpu.make_async_copy(early.at[pl.ds(0, NZC - 1)], early.at[pl.ds(0, NZC - 1)], side_sem.at[1]).wait()
        for peer in y_peers:
            pltpu.make_async_remote_copy(
                src_ref=early.at[:, :, peer],
                dst_ref=late.at[y],
                send_sem=side_sem.at[2],
                recv_sem=side_sem.at[3],
                device_id={"tbl": peer * NZC + zc},
                device_id_type=MESH,
            ).start()
        late[y] = early[:, :, y]


    for ch in range(1, AHEAD):
        dequantize(ch)
        send_y(ch)
    lax.fori_loop(AHEAD + 2, CHUNKS, lambda n, carry: (load_rows(n).start(), carry)[1], 0)
    dequantize(AHEAD)

    for load in loads:
        load.wait()
    row = lax.broadcasted_iota(jnp.int32, (SHIFTS * 32, PAIRS), 0)
    col = lax.broadcasted_iota(jnp.int32, (SHIFTS * 32, PAIRS), 1)
    first = row % 32
    second = first + row // 32 + 1
    second = jnp.where(second >= TABLES, second - TABLES, second)
    low = jnp.minimum(first, second)
    high = jnp.maximum(first, second)
    rank = low * TABLES - (low * (low + 1)) // 2 + high - low - 1
    chosen = jnp.where((rank == col) & (first < TABLES), 1.0, 0.0).astype(BF16)
    w1p[...] = jnp.dot(chosen, w1v[...], preferred_element_type=F32).astype(BF16)
    xt[...] = jnp.zeros_like(xt)
    acc[...] = jnp.zeros_like(acc)

    for load in slot_loads:
        load.wait()
    shard = lax.broadcasted_iota(jnp.int32, (56, NY * NZC), 0)
    table_row = lax.broadcasted_iota(jnp.int32, (56, NY * NZC), 1) % (2 * NZC)
    spot = table_row % NZC * 4 + table_row // NZC * 2
    place = jnp.zeros((56, 1), jnp.int32)
    for j in range(2):
        here = jnp.broadcast_to(slot_v[j : j + 1], shard.shape) == shard
        found = jnp.max(jnp.where(here, spot + j, 0), axis=1, keepdims=True)
        place = jnp.maximum(place, found)
    place_v[...] = jnp.broadcast_to(place, (56, 128))
    place_copy = pltpu.make_async_copy(place_v, place_s, slot_sem.at[0])
    place_copy.start()
    place_copy.wait()
    flags = [[slot_s[j, p * NZC + zc] for j in range(2)] for p in range(2)]

    def merge(ch):
        three = y_recv.at[ch, pl.ds(0, 3)]
        pltpu.make_async_copy(three, three, y_rsem.at[ch]).wait()
        for p in range(2):
            for j in range(2):
                merged[ch, :, p, j] = jnp.where(flags[p][j] >= 0, y_recv[ch, p, j], y_recv[ch, p + 2, j])
        for peer in z_peers:
            pltpu.make_async_remote_copy(
                src_ref=merged.at[ch, peer],
                dst_ref=z_recv.at[ch, zc],
                send_sem=z_ssem.at[ch],
                recv_sem=z_rsem.at[ch],
                device_id={"tbl": y * NZC + peer},
                device_id_type=MESH,
            ).start()
        z_recv[ch, zc] = merged[ch, zc]

    def gram(n):
        @pl.when(n != CHUNKS - 1)
        def _():
            ch = jnp.minimum(n, CHUNKS - 1)
            most = z_recv.at[ch, pl.ds(0, NZC - 1)]
            pltpu.make_async_copy(most, most, z_rsem.at[ch]).wait()

            def widen(s, carry):
                for half in range(2):
                    for p in range(2):
                        for j in range(2):
                            unit[s * 8 + half * 4 + p * 2 + j] = z_recv[ch, s * 2 + half, p, j].astype(F32)
                return carry

            lax.fori_loop(0, NZC // 2, widen, 0)

        @pl.when(n == CHUNKS - 1)
        def _():
            pltpu.make_async_copy(late.at[pl.ds(0, 3)], late.at[pl.ds(0, 3)], side_sem.at[3]).wait()

            def pick(s, carry):
                for p in range(2):
                    for j in range(2):
                        take_low = slot_s[j, p * NZC + s] >= 0
                        unit[s * 4 + p * 2 + j] = jnp.where(take_low, late[p, s, j], late[p + 2, s, j]).astype(F32)
                return carry

            lax.fori_loop(0, NZC, pick, 0)

        def place_three(b, carry):
            for r in range(3):
                t = b * 3 + r
                for h in range(2):
                    at = place_s[t * 2 + h, 0]
                    vals[h, t] = unit[at]
            return carry

        lax.fori_loop(0, TABLES // 3, place_three, 0)
        for h in range(2):
            vals[h, TABLES : TABLES + SHIFTS + 1] = vals[h, 0 : SHIFTS + 1]

        def shift(e, carry):
            d = e * 2
            for b in range(0, TABLES, 9):
                one = acc[d, b : b + 9]
                two = acc[d + 1, b : b + 9]
                for h in range(2):
                    left = vals[h, b : b + 9]
                    right = vals[h, pl.ds(d + 1 + b, 10)]
                    one = one + left * right[0:9]
                    two = two + left * right[1:10]
                acc[d, b : b + 9] = one
                acc[d + 1, b : b + 9] = two
            return carry

        lax.fori_loop(0, (SHIFTS + 1) // 2, shift, 0)

    def layer(inputs, weight, bias):
        product = jnp.dot(inputs, weight[...], preferred_element_type=F32)
        return jnp.maximum(product + bias[...], 0.0).astype(BF16)

    sub = lax.broadcasted_iota(jnp.int32, (8, 128), 0)

    def fold_rows(rows):
        for dist in (4, 2, 1):
            low = (sub & dist) == 0
            merged_rows = []
            for a in range(dist):
                one, two = rows[a], rows[a + dist]
                if one is None:
                    merged_rows.append(None)
                    continue
                two = jnp.zeros_like(one) if two is None else two
                other = jnp.where(low, two, one)
                if dist == 4:
                    moved = pltpu.roll(other, 4, 0)
                else:
                    moved = jnp.where(low, pltpu.roll(other, 8 - dist, 0), pltpu.roll(other, dist, 0))
                merged_rows.append(jnp.where(low, one, two) + moved)
            rows = merged_rows
        return rows[0]

    def finish(q):
        def fold(d, carry):
            for b in range(0, 32, 8):
                rows = [acc[d, b + r] if b + r < TABLES else None for r in range(8)]
                xt[pl.ds(pl.multiple_of(d * 32 + b, 8), 8)] = fold_rows(rows)
            acc[d] = jnp.zeros((TABLES, 8, 128), F32)
            return carry

        lax.fori_loop(0, SHIFTS, fold, 0)
        hidden = xt[...].T.astype(BF16)
        hidden = layer(hidden, w1p, b1v)
        hidden = layer(hidden, w2v, b2v)
        hidden = layer(hidden, w3v, b3v)
        hidden = layer(hidden, w4v, b4v)
        last = jnp.broadcast_to(woutv[...].astype(F32).reshape(1, 256), (8, 256)).astype(BF16)
        final = lax.dot_general(last, hidden, (((1,), (1,)), ((), ())), preferred_element_type=F32)
        lg[q] = final[0:1]
        out_ref[q, px] = final[0:1]
        for peer in x_peers:
            pltpu.make_async_remote_copy(
                src_ref=lg.at[q],
                dst_ref=out_ref.at[q, px],
                send_sem=lg_ssem.at[q],
                recv_sem=lg_rsem.at[q],
                device_id={"pair": peer},
                device_id_type=MESH,
            ).start()

    def step(i, carry):
        @pl.when(i < CHUNKS)
        def _():
            merge(i)

        @pl.when(i + AHEAD < CHUNKS)
        def _():
            send_y(i + AHEAD)

        @pl.when(i + AHEAD + 1 < CHUNKS)
        def _():
            dequantize(i + AHEAD + 1)

        @pl.when(i + AHEAD == CHUNKS)
        def _():
            send_late()

        @pl.when(i >= LAG)
        def _():
            gram(i - LAG)

        @pl.when((i >= LAG) & ((i - LAG) % NG == NG - 1))
        def _():
            finish((i - LAG) // NG)

        return carry

    lax.fori_loop(0, GROUPS + LAG, step, 0)

    def sent(ch, carry):
        three = y_recv.at[ch, pl.ds(0, 3)]
        pltpu.make_async_copy(three, three, y_ssem.at[ch]).wait()
        most = z_recv.at[ch, pl.ds(0, NZC - 1)]
        pltpu.make_async_copy(most, most, z_ssem.at[ch]).wait()
        return carry

    lax.fori_loop(0, CHUNKS, sent, 0)
    pltpu.make_async_copy(early.at[pl.ds(0, NZC - 1)], early.at[pl.ds(0, NZC - 1)], side_sem.at[0]).wait()
    pltpu.make_async_copy(late.at[pl.ds(0, 3)], late.at[pl.ds(0, 3)], side_sem.at[2]).wait()
    for q in range(NQ):
        three = out_ref.at[q, pl.ds(0, 3)]
        pltpu.make_async_copy(three, three, lg_ssem.at[q]).wait()
        pltpu.make_async_copy(three, three, lg_rsem.at[q]).wait()


def per_device(codes, scales, shard_slot, w1, b1, w2, b2, w3, b3, w4, b4, wout, bout):
    codes = codes.reshape(2, NG, 8, NY, NZC, NQ, 128).transpose(0, 1, 3, 4, 5, 2, 6)
    scales = scales.reshape(2, NY * NZC, NQ, 128).transpose(1, 2, 0, 3).reshape(NY * NZC, 8, 128)

    any_spec = pl.BlockSpec(memory_space=pl.ANY)
    dma = pltpu.SemaphoreType.DMA
    logits = pl.pallas_call(
        kernel,
        out_shape=pltpu.VMEM((NQ, NX, 1, 128), F32),
        in_specs=[any_spec] * 12,
        out_specs=pl.BlockSpec(memory_space=pltpu.VMEM),
        scratch_shapes=[
            pltpu.VMEM((2, NY * NZC), jnp.int32),
            pltpu.SMEM((2, NY * NZC), jnp.int32),
            pltpu.VMEM((56, 128), jnp.int32),
            pltpu.SMEM((56, 128), jnp.int32),
            pltpu.VMEM(wout.shape, BF16),
            pltpu.VMEM((CHUNKS, NY, 2, NZC, 8, 128), BF16),
            pltpu.VMEM((CHUNKS, NZC, 2, 2, 8, 128), BF16),
            pltpu.VMEM((CHUNKS, NZC, 2, 2, 8, 128), BF16),
            pltpu.VMEM((NZC, 2, NY, 8, 128), BF16),
            pltpu.VMEM((NY, NZC, 2, 8, 128), BF16),
            pltpu.VMEM((NY * NZC, 8, 128), F32),
            pltpu.VMEM((GROUPS, 2, NY, NZC, 8, 128), BF16),
            pltpu.VMEM((64, 8, 128), F32),
            pltpu.VMEM((2, TABLES + SHIFTS + 1, 8, 128), F32),
            pltpu.VMEM((SHIFTS + 1, TABLES, 8, 128), F32),
            pltpu.VMEM((SHIFTS * 32, 128), F32),
            pltpu.VMEM((NQ, 1, 128), F32),
            pltpu.VMEM(w1.shape, BF16),
            pltpu.VMEM((SHIFTS * 32, w1.shape[1]), BF16),
            pltpu.VMEM((1, b1.shape[0]), F32),
            pltpu.VMEM(w2.shape, BF16),
            pltpu.VMEM((1, b2.shape[0]), F32),
            pltpu.VMEM(w3.shape, BF16),
            pltpu.VMEM((1, b3.shape[0]), F32),
            pltpu.VMEM(w4.shape, BF16),
            pltpu.VMEM((1, b4.shape[0]), F32),
            dma((CHUNKS,)),
            dma((CHUNKS,)),
            dma((CHUNKS,)),
            dma((CHUNKS,)),
            dma((GROUPS,)),
            dma((NQ,)),
            dma((NQ,)),
            dma((4,)),
            dma,
            dma((2,)),
            dma((9,)),
        ],
        compiler_params=pltpu.CompilerParams(
            collective_id=0, has_side_effects=True, vmem_limit_bytes=56 * 1024 * 1024
        ),
    )(shard_slot.T, codes, scales, w1, b1[None], w2, b2[None], w3, b3[None], w4, b4[None], wout)
    return logits.transpose(1, 2, 0, 3).reshape(NX, NQ * 128) + bout


def solution(mesh):
    return jax.shard_map(
        per_device,
        mesh=mesh,
        in_specs=(P("tbl", None, "pair"), P("tbl", "pair")) + (P(),) * 11,
        out_specs=P(None, "tbl"),
        check_vma=False,
    )
```
